16 devices in a mesh: ep: 16 (over z, y, x, core).
Axes of the slice: x: 2, y: 2, z: 2, core: 2. Of those that a mesh axis runs over, the one named last changes fastest.
Arguments:
- x_tokens: bfloat16 [32768, 1024], P('ep')
- w_router: bfloat16 [1024, 32], replicated
- w_gate: bfloat16 [32, 1024, 512], P('ep')
- w_up: bfloat16 [32, 1024, 512], P('ep')
- w_down: bfloat16 [32, 512, 1024], P('ep')
- topk_idx: int32 [32768, 8], P('ep')
- dy_tokens: bfloat16 [32768, 1024], P('ep')
Outputs:
- output 1: bfloat16 [32768, 1024], P('ep')
- output 2: float32 [], replicated
- output 3: bfloat16 [32768, 1024], P('ep')
- output 4: float32 [1024, 32], replicated
- output 5: float32 [32, 1024, 512], P('ep')
- output 6: float32 [32, 1024, 512], P('ep')
- output 7: float32 [32, 512, 1024], P('ep')
All inputs are finite; a program needn't handle non-finite values.
Results may differ from the reference program's by a relative error of at most 0.00538827.
Values are sent between devices in bfloat16 or wider.
A program may use at most 1 GiB of HBM per device.

```python
import jax
import jax.numpy as jnp
from jax import lax

MODEL_DIM = 1024
FF_DIM = 512
NUM_EXPERTS = 32
TOP_K = 8
TOK_PER_DEV = 2048
NUM_DEVICES = 16
ALL_TOKENS = NUM_DEVICES * TOK_PER_DEV
CAPACITY = (5 * TOK_PER_DEV * TOP_K + 4 * NUM_EXPERTS - 1) // (4 * NUM_EXPERTS)
AUX_COEF = 0.001


def draw_routing(key):
    bias_key, score_key = jax.random.split(key)
    dev_bias = jax.random.randint(bias_key, (NUM_DEVICES, 1, NUM_EXPERTS), 0, 61)
    scores = jax.random.randint(score_key, (NUM_DEVICES, TOK_PER_DEV, NUM_EXPERTS), 0, 1000)
    ranked = (scores + dev_bias) * NUM_EXPERTS + jnp.arange(NUM_EXPERTS, dtype=jnp.int32)
    chosen = lax.top_k(ranked, TOP_K)[1]
    return chosen.reshape(ALL_TOKENS, TOP_K).astype(jnp.int32)


def setup_inputs(seed: int = 0) -> dict:
    key_list = jax.random.split(jax.random.key(seed), 7)
    topk_idx = draw_routing(key_list[0])
    router_f = jax.random.normal(key_list[1], (MODEL_DIM, NUM_EXPERTS), jnp.float32) * MODEL_DIM ** -0.5
    chosen_hot = jnp.zeros((ALL_TOKENS, NUM_EXPERTS), jnp.float32).at[jnp.arange(ALL_TOKENS)[:, None], topk_idx].set(1.0)
    x_noise = jax.random.normal(key_list[2], (ALL_TOKENS, MODEL_DIM), jnp.float32)
    x_tokens = x_noise + 3.0 * jnp.dot(chosen_hot, router_f.T)
    w_gate = jax.random.normal(key_list[3], (NUM_EXPERTS, MODEL_DIM, FF_DIM), jnp.float32) * MODEL_DIM ** -0.5
    w_up = jax.random.normal(key_list[4], (NUM_EXPERTS, MODEL_DIM, FF_DIM), jnp.float32) * MODEL_DIM ** -0.5
    w_down = jax.random.normal(key_list[5], (NUM_EXPERTS, FF_DIM, MODEL_DIM), jnp.float32) * FF_DIM ** -0.5
    dy_tokens = jax.random.normal(key_list[6], (ALL_TOKENS, MODEL_DIM), jnp.float32)
    return {
        "x_tokens": x_tokens.astype(jnp.bfloat16),
        "w_router": router_f.astype(jnp.bfloat16),
        "w_gate": w_gate.astype(jnp.bfloat16),
        "w_up": w_up.astype(jnp.bfloat16),
        "w_down": w_down.astype(jnp.bfloat16),
        "topk_idx": topk_idx,
        "dy_tokens": dy_tokens.astype(jnp.bfloat16),
    }


def reference(x_tokens, w_router, w_gate, w_up, w_down, topk_idx, dy_tokens):
    logits = jnp.dot(x_tokens, w_router, preferred_element_type=jnp.float32)
    router_prob = jax.nn.softmax(logits, axis=-1)
    counts = jax.ops.segment_sum(jnp.ones((ALL_TOKENS * TOP_K,), jnp.float32), topk_idx.reshape(-1), num_segments=NUM_EXPERTS)
    load_frac = counts / (ALL_TOKENS * TOP_K)
    mean_prob = jnp.mean(router_prob, axis=0)
    aux_loss = AUX_COEF * NUM_EXPERTS * jnp.sum(load_frac * mean_prob)
    aux_grad = AUX_COEF * NUM_EXPERTS * load_frac / ALL_TOKENS
    w_gate32 = w_gate.astype(jnp.float32)
    w_up32 = w_up.astype(jnp.float32)
    w_down32 = w_down.astype(jnp.float32)
    zero_row = jnp.zeros((1, MODEL_DIM), x_tokens.dtype)
    n_slots = NUM_EXPERTS * CAPACITY

    def device_step(carry_acc, dev_in):
        dwg_acc, dwu_acc, dwd_acc, dwr_acc = carry_acc
        x_dev, prob_dev, idx_dev, dy_dev = dev_in
        pick_prob = jnp.take_along_axis(prob_dev, idx_dev, axis=1)
        pick_sum = jnp.sum(pick_prob, axis=1, keepdims=True)
        gate_f32 = pick_prob / pick_sum
        gate_bf = gate_f32.astype(jnp.bfloat16)
        choice_mask = idx_dev[:, :, None] == jnp.arange(NUM_EXPERTS)[None, None, :]
        expert_hot = jnp.sum(choice_mask.astype(jnp.int32), axis=1)
        earlier = jnp.cumsum(expert_hot, axis=0) - expert_hot
        position = jnp.take_along_axis(earlier, idx_dev, axis=1)
        slot_ids = jnp.where(position < CAPACITY, idx_dev * CAPACITY + position, n_slots)
        flat_slots = slot_ids.reshape(-1)
        x_rep = jnp.broadcast_to(x_dev[:, None, :], (TOK_PER_DEV, TOP_K, MODEL_DIM)).reshape(TOK_PER_DEV * TOP_K, MODEL_DIM)
        buf_x = jnp.zeros((n_slots + 1, MODEL_DIM), x_dev.dtype).at[flat_slots].set(x_rep)[:n_slots]
        buf_x32 = buf_x.reshape(NUM_EXPERTS, CAPACITY, MODEL_DIM).astype(jnp.float32)
        gate_pre = jnp.einsum("ecd,edf->ecf", buf_x32, w_gate32)
        up_pre = jnp.einsum("ecd,edf->ecf", buf_x32, w_up32)
        act_gate = jax.nn.silu(gate_pre)
        hidden = (act_gate * up_pre).astype(jnp.bfloat16).astype(jnp.float32)
        out_slot = jnp.einsum("ecf,efd->ecd", hidden, w_down32).astype(jnp.bfloat16)
        out_tok = jnp.concatenate([out_slot.reshape(n_slots, MODEL_DIM), zero_row])[slot_ids]
        y_dev = jnp.sum(gate_bf.astype(jnp.float32)[:, :, None] * out_tok.astype(jnp.float32), axis=1).astype(jnp.bfloat16)
        do_tok = (gate_bf.astype(jnp.float32)[:, :, None] * dy_dev.astype(jnp.float32)[:, None, :]).astype(jnp.bfloat16)
        buf_do = jnp.zeros((n_slots + 1, MODEL_DIM), dy_dev.dtype).at[flat_slots].set(do_tok.reshape(TOK_PER_DEV * TOP_K, MODEL_DIM))[:n_slots]
        buf_do32 = buf_do.reshape(NUM_EXPERTS, CAPACITY, MODEL_DIM).astype(jnp.float32)
        dwd_new = dwd_acc + jnp.einsum("ecf,ecd->efd", hidden, buf_do32)
        d_hidden = jnp.einsum("ecd,efd->ecf", buf_do32, w_down32).astype(jnp.bfloat16).astype(jnp.float32)
        sigmoid_g = jax.nn.sigmoid(gate_pre)
        d_gate_pre = (d_hidden * up_pre * sigmoid_g * (1.0 + gate_pre * (1.0 - sigmoid_g))).astype(jnp.bfloat16).astype(jnp.float32)
        d_up_pre = (d_hidden * act_gate).astype(jnp.bfloat16).astype(jnp.float32)
        dwg_new = dwg_acc + jnp.einsum("ecd,ecf->edf", buf_x32, d_gate_pre)
        dwu_new = dwu_acc + jnp.einsum("ecd,ecf->edf", buf_x32, d_up_pre)
        dx_slot = (jnp.einsum("ecf,edf->ecd", d_gate_pre, w_gate32) + jnp.einsum("ecf,edf->ecd", d_up_pre, w_up32)).astype(jnp.bfloat16)
        dx_tok = jnp.concatenate([dx_slot.reshape(n_slots, MODEL_DIM), zero_row])[slot_ids]
        dx_expert = jnp.sum(dx_tok.astype(jnp.float32), axis=1)
        d_gate = jnp.sum(out_tok.astype(jnp.float32) * dy_dev.astype(jnp.float32)[:, None, :], axis=2)
        d_pick = (d_gate - jnp.sum(d_gate * gate_f32, axis=1, keepdims=True)) / pick_sum
        d_prob = jnp.sum(jnp.where(choice_mask, d_pick[:, :, None], 0.0), axis=1) + aux_grad
        d_logit = prob_dev * (d_prob - jnp.sum(prob_dev * d_prob, axis=1, keepdims=True))
        d_logit_bf = d_logit.astype(jnp.bfloat16)
        dwr_new = dwr_acc + jnp.dot(x_dev.T, d_logit_bf, preferred_element_type=jnp.float32)
        dx_dev = (dx_expert + jnp.dot(d_logit_bf, w_router.T, preferred_element_type=jnp.float32)).astype(jnp.bfloat16)
        return (dwg_new, dwu_new, dwd_new, dwr_new), (y_dev, dx_dev)

    init_acc = (
        jnp.zeros((NUM_EXPERTS, MODEL_DIM, FF_DIM), jnp.float32),
        jnp.zeros((NUM_EXPERTS, MODEL_DIM, FF_DIM), jnp.float32),
        jnp.zeros((NUM_EXPERTS, FF_DIM, MODEL_DIM), jnp.float32),
        jnp.zeros((MODEL_DIM, NUM_EXPERTS), jnp.float32),
    )
    dev_inputs = (
        x_tokens.reshape(NUM_DEVICES, TOK_PER_DEV, MODEL_DIM),
        router_prob.reshape(NUM_DEVICES, TOK_PER_DEV, NUM_EXPERTS),
        topk_idx.reshape(NUM_DEVICES, TOK_PER_DEV, TOP_K),
        dy_tokens.reshape(NUM_DEVICES, TOK_PER_DEV, MODEL_DIM),
    )
    final_acc, dev_outs = lax.scan(device_step, init_acc, dev_inputs)
    y_tokens = dev_outs[0].reshape(ALL_TOKENS, MODEL_DIM)
    dx_tokens = dev_outs[1].reshape(ALL_TOKENS, MODEL_DIM)
    return (y_tokens, aux_loss, dx_tokens, final_acc[3], final_acc[0], final_acc[1], final_acc[2])
```

```python
import functools

import jax
import jax.numpy as jnp
from jax import lax
from jax.experimental import pallas as pl
from jax.experimental.pallas import tpu as pltpu
from jax.sharding import PartitionSpec as P

AUX_COEF = 0.001
SEG = 512
WIN = 192
TILE = 640
F32, BF16 = jnp.float32, jnp.bfloat16


def mm(a, b, ca=1, cb=0):
    return lax.dot_general(a, b, (((ca,), (cb,)), ((), ())), preferred_element_type=F32)


def window(cnt_ref, row, b):
    start = (cnt_ref[row, b] // 16) * 16
    return pl.multiple_of(start, 16), jnp.maximum((cnt_ref[row, b + 1] - start + WIN - 1) // WIN, 1)


def hot_rows(pos_ref, b, start):
    pos = pos_ref[0, :, b * SEG:(b + 1) * SEG] - start
    return lax.broadcasted_iota(jnp.int32, (WIN, SEG), 0) == pos


def gather_rows(cnt_ref, row, pos_ref, w_ref, x_ref, dy_ref, xs, dys, ds, n_seg, n_rows):
    end = 0
    for b in range(n_seg):
        first, n_win = window(cnt_ref, row, b)

        def step(c, _, b=b, first=first):
            start = pl.multiple_of(first + c * WIN, 16)
            hot = hot_rows(pos_ref, b, start)
            sel = hot.astype(F32).astype(BF16)
            tok = slice(b * SEG, (b + 1) * SEG)
            w_col = jnp.sum(jnp.where(hot, w_ref[0, :, tok], 0.0), axis=1, keepdims=True)
            x_new = mm(sel, x_ref[tok, :])
            dy_new = mm(sel, dy_ref[tok, :])
            d_new = w_col * dy_new
            outs = [(xs, x_new), (ds, d_new)] + ([(dys, dy_new)] if dys is not None else [])
            for ref, new in outs:
                new = new.astype(BF16)
                ref[pl.ds(start + 16, WIN - 16), :] = new[16:]
                if b == 0:
                    ref[pl.ds(start, 16), :] = new[:16]
                else:
                    old = ref[pl.ds(start, 16), :].astype(F32)
                    keep = jnp.where(c == 0, 1.0, 0.0)
                    ref[pl.ds(start, 16), :] = (jnp.where(keep > 0, old, 0.0) + new[:16].astype(F32)).astype(BF16)
            return 0

        step(0, 0)
        lax.fori_loop(1, n_win, step, 0)
        end = first + n_win * WIN

    def clear(i, _):
        at = pl.multiple_of(i * 16, 16)
        zero = jnp.zeros((16, xs.shape[1]), BF16)
        xs[pl.ds(at, 16), :] = zero
        ds[pl.ds(at, 16), :] = zero
        if dys is not None:
            dys[pl.ds(at, 16), :] = zero
        return 0

    lax.fori_loop(end // 16, n_rows // 16, clear, 0)


def slot_grads(x, d, wg, wu, wd):
    g = mm(x, wg)
    u = mm(x, wu)
    s = jax.nn.sigmoid(g)
    act = g * s
    h = (act * u).astype(BF16)
    dh = mm(d, wd, 1, 1).astype(BF16).astype(F32)
    dg = (dh * u * s * (1.0 + g * (1.0 - s))).astype(BF16)
    du = (dh * act).astype(BF16)
    return h, dg, du


def token_kernel(first, cnt_ref, pos_ref, w_ref, x_ref, dy_ref, wg_ref, wu_ref, wd_ref, y_in, dx_in,
                 y_out, dx_out, a_out, xs, dys, ds, os, dxs, y_acc, dx_acc, sems):
    i = pl.program_id(0)
    n_seg = x_ref.shape[0] // SEG

    @pl.when(i == 0)
    def _():
        if first:
            y_acc[...] = jnp.zeros_like(y_acc)
            dx_acc[...] = jnp.zeros_like(dx_acc)
        else:
            loads = [pltpu.make_async_copy(y_in, y_acc, sems.at[0]), pltpu.make_async_copy(dx_in, dx_acc, sems.at[1])]
            for copy in loads:
                copy.start()
            for copy in loads:
                copy.wait()
        os[...] = jnp.zeros_like(os)
        dxs[...] = jnp.zeros_like(dxs)

    gather_rows(cnt_ref, i, pos_ref, w_ref, x_ref, dy_ref, xs, dys, ds, n_seg, TILE)
    h, dg, du = slot_grads(xs[:TILE, :], ds[:TILE, :], wg_ref[0], wu_ref[0], wd_ref[0])
    o = mm(h, wd_ref[0]).astype(BF16)
    os[:TILE, :] = o
    dxs[:TILE, :] = (mm(dg, wg_ref[0], 1, 1) + mm(du, wu_ref[0], 1, 1)).astype(BF16)

    for b in range(n_seg):
        start0, n_win = window(cnt_ref, i, b)
        tok = slice(b * SEG, (b + 1) * SEG)

        def step(c, a_row, b=b, start0=start0, tok=tok):
            start = pl.multiple_of(start0 + c * WIN, 16)
            hot = hot_rows(pos_ref, b, start)
            sel = hot.astype(F32)
            sel_w = jnp.where(hot, w_ref[0, :, tok], 0.0).astype(BF16)
            o_win = os[pl.ds(start, WIN), :]
            y_acc[tok, :] += mm(sel_w, o_win, 0, 0)
            dx_acc[tok, :] += mm(sel.astype(BF16), dxs[pl.ds(start, WIN), :], 0, 0)
            a_col = jnp.sum(o_win.astype(F32) * dys[pl.ds(start, WIN), :].astype(F32), axis=1, keepdims=True)
            return a_row + jnp.sum(jnp.where(hot, a_col, 0.0), axis=0, keepdims=True)

        a_row = step(0, jnp.zeros((1, SEG), F32))
        a_out[0, :, tok] = lax.fori_loop(1, n_win, step, a_row)

    @pl.when(i == pl.num_programs(0) - 1)
    def _():
        stores = [pltpu.make_async_copy(y_acc, y_out, sems.at[0]), pltpu.make_async_copy(dx_acc, dx_out, sems.at[1])]
        for copy in stores:
            copy.start()
        for copy in stores:
            copy.wait()


def token_side(first, cnt, pos, w, x, dy, wg, wu, wd, y_in, dx_in):
    n_exp, _, tok_count = pos.shape
    dim, ff = wg.shape[1:]
    whole = lambda shape: pl.BlockSpec(shape, lambda i, c: (0,) * len(shape), pipeline_mode=pl.Buffered(1))
    per_exp = lambda shape: pl.BlockSpec((1,) + shape, lambda i, c: (i, 0, 0))
    any_spec = pl.BlockSpec(memory_space=pl.ANY)
    acc_shape = jax.ShapeDtypeStruct((tok_count, dim), F32)
    return pl.pallas_call(
        functools.partial(token_kernel, first),
        grid_spec=pltpu.PrefetchScalarGridSpec(
            num_scalar_prefetch=1,
            grid=(n_exp,),
            in_specs=[per_exp((1, tok_count)), per_exp((1, tok_count)), whole((tok_count, dim)), whole((tok_count, dim)),
                      per_exp((dim, ff)), per_exp((dim, ff)), per_exp((ff, dim)), any_spec, any_spec],
            out_specs=[any_spec, any_spec, per_exp((1, tok_count))],
            scratch_shapes=[pltpu.VMEM((TILE + WIN, dim), BF16)] * 5 + [pltpu.VMEM((tok_count, dim), F32)] * 2
            + [pltpu.SemaphoreType.DMA((2,))],
        ),
        out_shape=[acc_shape, acc_shape, jax.ShapeDtypeStruct((n_exp, 1, tok_count), F32)],
        input_output_aliases={} if first else {8: 0, 9: 1},
        compiler_params=pltpu.CompilerParams(dimension_semantics=("arbitrary",), vmem_limit_bytes=67000000),
        cost_estimate=pl.CostEstimate(flops=n_exp * 12 * 640 * dim * ff * 2, bytes_accessed=100 << 20, transcendentals=0),
        name="token_side",
    )(cnt, pos, w, x, dy, wg, wu, wd, y_in, dx_in)


def owner_kernel(first, cnt_ref, pos_ref, w_ref, x_ref, dy_ref, wg_ref, wu_ref, wd_ref, ag_in, au_in, ad_in,
                 ag_out, au_out, ad_out, xs, ds, ag, au, ad, sems):
    g, e = pl.program_id(0), pl.program_id(1)
    n_grp, n_exp = pl.num_programs(0), pl.num_programs(1)
    n_seg = x_ref.shape[0] // SEG
    row = g * n_exp + e
    accs = (ag, au, ad)

    @pl.when((g == 0) & (e == 0))
    def _():
        if first:
            for acc in accs:
                acc[...] = jnp.zeros_like(acc)
        else:
            loads = [pltpu.make_async_copy(src, acc, sems.at[k]) for k, (src, acc) in enumerate(zip((ag_in, au_in, ad_in), accs))]
            for copy in loads:
                copy.start()
            for copy in loads:
                copy.wait()

    n_tile = (cnt_ref[row, n_seg] + TILE - 1) // TILE
    gather_rows(cnt_ref, row, pos_ref, w_ref, x_ref, dy_ref, xs, None, ds, n_seg, n_tile * TILE)

    def tile(t, _):
        at = pl.multiple_of(t * TILE, 16)
        x, d = xs[pl.ds(at, TILE), :], ds[pl.ds(at, TILE), :]
        h, dg, du = slot_grads(x, d, wg_ref[0], wu_ref[0], wd_ref[0])
        ad[e] += mm(h, d, 0, 0)
        ag[e] += mm(x, dg, 0, 0)
        au[e] += mm(x, du, 0, 0)
        return 0

    lax.fori_loop(0, n_tile, tile, 0)

    @pl.when((g == n_grp - 1) & (e == n_exp - 1))
    def _():
        stores = [pltpu.make_async_copy(acc, dst, sems.at[k]) for k, (dst, acc) in enumerate(zip((ag_out, au_out, ad_out), accs))]
        for copy in stores:
            copy.start()
        for copy in stores:
            copy.wait()


def owner_side(first, cnt, pos, w, x, dy, wg, wu, wd, accs):
    n_exp, dim, ff = wg.shape
    grp = pos.shape[2]
    n_grp = x.shape[0] // grp
    per_row = pl.BlockSpec((1, 1, grp), lambda g, e, c: (g * n_exp + e, 0, 0))
    per_grp = pl.BlockSpec((grp, dim), lambda g, e, c: (g, 0))
    per_exp = lambda shape: pl.BlockSpec((1,) + shape, lambda g, e, c: (e, 0, 0))
    any_spec = pl.BlockSpec(memory_space=pl.ANY)
    rows = -(-grp // TILE) * TILE + WIN
    return pl.pallas_call(
        functools.partial(owner_kernel, first),
        grid_spec=pltpu.PrefetchScalarGridSpec(
            num_scalar_prefetch=1,
            grid=(n_grp, n_exp),
            in_specs=[per_row, per_row, per_grp, per_grp, per_exp((dim, ff)), per_exp((dim, ff)), per_exp((ff, dim))]
            + [any_spec] * 3,
            out_specs=[any_spec] * 3,
            scratch_shapes=[pltpu.VMEM((rows, dim), BF16)] * 2
            + [pltpu.VMEM((n_exp, dim, ff), F32)] * 2 + [pltpu.VMEM((n_exp, ff, dim), F32), pltpu.SemaphoreType.DMA((3,))],
        ),
        out_shape=[jax.ShapeDtypeStruct(a.shape, F32) for a in accs],
        input_output_aliases={} if first else {8: 0, 9: 1, 10: 2},
        compiler_params=pltpu.CompilerParams(dimension_semantics=("arbitrary", "arbitrary"), vmem_limit_bytes=67000000),
        cost_estimate=pl.CostEstimate(flops=n_grp * n_exp * 12 * 640 * dim * ff * 2, bytes_accessed=100 << 20, transcendentals=0),
        name="owner_side",
    )(cnt, pos, w, x, dy, wg, wu, wd, *accs)


def running_count(hot):
    rows, width = hot.shape
    blocks = hot.reshape(rows, width // 256, 256)
    upper = (jnp.arange(256)[:, None] < jnp.arange(256)[None, :]).astype(BF16)
    inside = jnp.einsum("rbi,ij->rbj", blocks.astype(BF16), upper, preferred_element_type=F32)
    total = jnp.sum(blocks, axis=2)
    n_blk = width // 256
    before = jnp.sum(jnp.where(jnp.arange(n_blk)[:, None] < jnp.arange(n_blk + 1)[None, :], total[:, :, None], 0.0), axis=1)
    return (inside + before[:, :-1, None]).reshape(rows, width), before[:, ::SEG // 256]


def solution(mesh):
    n_dev = mesh.shape["ep"]

    def local_block(x_loc, w_router, wg_loc, wu_loc, wd_loc, idx_loc, dy_loc):
        tok_count, dim = x_loc.shape
        top_k = idx_loc.shape[1]
        n_exp = w_router.shape[1]
        loc_exp = wg_loc.shape[0]
        capacity = (5 * tok_count * top_k + 4 * n_exp - 1) // (4 * n_exp)
        n_total = tok_count * n_dev
        n_chunk = 2
        span = tok_count // n_chunk
        gather = lambda a: lax.all_gather(a, "ep", axis=0, tiled=True)

        w_all = [gather(a) for a in (wg_loc, wu_loc, wd_loc)]
        tok_all = [[gather(a[c * span:(c + 1) * span]) for a in (x_loc, dy_loc)] for c in range(n_chunk)]

        idx_t = idx_loc.T
        exp_id = jnp.arange(n_exp, dtype=jnp.int32)[:, None]
        hot = exp_id == idx_t[0:1]
        for k in range(1, top_k):
            hot = hot | (exp_id == idx_t[k:k + 1])
        logits = lax.dot_general(w_router, x_loc, (((0,), (1,)), ((), ())), preferred_element_type=F32)
        prob = jax.nn.softmax(logits, axis=0)
        pick_sum = jnp.sum(jnp.where(hot, prob, 0.0), axis=0, keepdims=True)
        gate = jnp.where(hot, prob / pick_sum, 0.0)
        gate_bf = lax.reduce_precision(gate, 8, 7)
        earlier, before = running_count(hot.astype(F32))
        kept = hot & (earlier < capacity)
        pos = jnp.where(kept, earlier, -1.0).astype(jnp.int32)[:, None, :]
        cnt = jnp.minimum(before, capacity).astype(jnp.int32)

        y_acc = dx_acc = jnp.zeros((8, 128), F32)
        y_acc, dx_acc, a = token_side(True, cnt, pos, gate_bf[:, None, :], x_loc, dy_loc, *w_all, y_acc, dx_acc)
        a = a[:, 0]

        sent = jnp.where(kept, gate_bf, -1.0).reshape(n_dev, loc_exp, tok_count)
        got = lax.all_to_all(sent, "ep", 0, 0).reshape(n_dev, loc_exp, n_chunk, span)
        per_grp = n_chunk
        got = got.reshape(n_dev // per_grp, per_grp, loc_exp, n_chunk, span).transpose(3, 0, 2, 1, 4)
        got = got.reshape(-1, tok_count)
        own_hot = got >= 0.0
        own_pos, own_cnt = running_count(own_hot.astype(F32))
        own_pos = jnp.where(own_hot, own_pos, -1.0).astype(jnp.int32)[:, None, :]
        own_cnt = own_cnt.astype(jnp.int32)
        own_w = jnp.where(own_hot, got, 0.0)[:, None, :]
        accs = [jnp.zeros(a.shape, F32) for a in (wg_loc, wu_loc, wd_loc)]
        n_row = own_pos.shape[0] // n_chunk
        for c in range(n_chunk):
            part = slice(c * n_row, (c + 1) * n_row)
            accs = owner_side(c == 0, own_cnt[part], own_pos[part], own_w[part], *tok_all[c], wg_loc, wu_loc, wd_loc, accs)
        dw_gate, dw_up, dw_down = accs

        load_stats = jnp.concatenate([jnp.sum(hot.astype(F32), axis=1), jnp.sum(prob, axis=1)])
        load_stats = lax.psum(load_stats, "ep")
        load_frac = load_stats[:n_exp] / (n_total * top_k)
        mean_prob = load_stats[n_exp:] / n_total
        aux_loss = AUX_COEF * n_exp * jnp.sum(load_frac * mean_prob)

        d_pick = (a - jnp.sum(a * gate, axis=0, keepdims=True)) / pick_sum
        d_prob = jnp.where(hot, d_pick, 0.0) + (AUX_COEF * n_exp / n_total) * load_frac[:, None]
        d_logit = (prob * (d_prob - jnp.sum(prob * d_prob, axis=0, keepdims=True))).astype(BF16)
        dw_router = lax.dot_general(x_loc, d_logit, (((0,), (1,)), ((), ())), preferred_element_type=F32)
        dw_router = lax.psum(dw_router, "ep")
        dx_router = lax.dot_general(d_logit, w_router, (((0,), (1,)), ((), ())), preferred_element_type=F32)
        return y_acc.astype(BF16), aux_loss, (dx_acc + dx_router).astype(BF16), dw_router, dw_gate, dw_up, dw_down

    tok_spec = P("ep")
    return jax.shard_map(
        local_block,
        mesh=mesh,
        in_specs=(tok_spec, P(), tok_spec, tok_spec, tok_spec, tok_spec, tok_spec),
        out_specs=(tok_spec, P(), tok_spec, P(), tok_spec, tok_spec, tok_spec),
        check_vma=False,
    )
```

```python
import functools

import jax
import jax.numpy as jnp
from jax import lax
from jax.experimental import pallas as pl
from jax.experimental.pallas import tpu as pltpu
from jax.sharding import PartitionSpec as P


AUX_COEF = 0.001
SEG = 512
WIN = 192
TILE = 640
EAGER = True
F32, BF16 = jnp.float32, jnp.bfloat16


def mm(a, b, ca=1, cb=0):
    return lax.dot_general(a, b, (((ca,), (cb,)), ((), ())), preferred_element_type=F32)


def window(cnt_ref, row, b):
    start = (cnt_ref[row, b] // 16) * 16
    return pl.multiple_of(start, 16), jnp.maximum((cnt_ref[row, b + 1] - start + WIN - 1) // WIN, 1)


def hot_rows(pos_ref, b, start):
    pos = pos_ref[0, :, b * SEG:(b + 1) * SEG] - start
    return lax.broadcasted_iota(jnp.int32, (WIN, SEG), 0) == pos


def gather_rows(cnt_ref, row, pos_ref, w_ref, t_ref, xs, dys, ds, n_seg, n_rows):
    dim = xs.shape[1]
    end = 0
    for b in range(n_seg):
        first, n_win = window(cnt_ref, row, b)

        def step(c, _, b=b, first=first):
            start = pl.multiple_of(first + c * WIN, 16)
            hot = hot_rows(pos_ref, b, start)
            sel = hot.astype(F32).astype(BF16)
            tok = slice(b * SEG, (b + 1) * SEG)
            w_col = jnp.sum(jnp.where(hot, w_ref[0, :, tok], 0.0), axis=1, keepdims=True)
            both = mm(sel, t_ref[tok, :])
            x_new, dy_new = both[:, :dim], both[:, dim:]
            d_new = w_col * dy_new
            outs = [(xs, x_new), (ds, d_new)] + ([(dys, dy_new)] if dys is not None else [])
            for ref, new in outs:
                new = new.astype(BF16)
                ref[pl.ds(start + 16, WIN - 16), :] = new[16:]
                if b == 0:
                    ref[pl.ds(start, 16), :] = new[:16]
                else:
                    old = ref[pl.ds(start, 16), :].astype(F32)
                    keep = jnp.where(c == 0, 1.0, 0.0)
                    ref[pl.ds(start, 16), :] = (jnp.where(keep > 0, old, 0.0) + new[:16].astype(F32)).astype(BF16)
            return 0

        if EAGER:
            step(0, 0)
        lax.fori_loop(int(EAGER), n_win, step, 0)
        end = first + n_win * WIN

    def clear(i, _):
        at = pl.multiple_of(i * 16, 16)
        zero = jnp.zeros((16, dim), BF16)
        xs[pl.ds(at, 16), :] = zero
        ds[pl.ds(at, 16), :] = zero
        if dys is not None:
            dys[pl.ds(at, 16), :] = zero
        return 0

    lax.fori_loop(end // 16, n_rows // 16, clear, 0)


def slot_grads(x, d, w_ref, dim):
    pre = mm(x, w_ref[0, :dim, :])
    ff = pre.shape[1] // 2
    g, u = pre[:, :ff], pre[:, ff:]
    s = jax.nn.sigmoid(g)
    act = g * s
    h = (act * u).astype(BF16)
    dh = mm(d, w_ref[0, dim:, :], 1, 1).astype(BF16).astype(F32)
    dg = (dh * u * s * (1.0 + g * (1.0 - s))).astype(BF16)
    du = (dh * act).astype(BF16)
    return h, jnp.concatenate([dg, du], axis=1)


def token_kernel(first, counts, id_ref, src_ref, cnt_ref, pos_ref, w_ref, t_ref, *refs):
    n_src = len(counts)
    wt_refs = refs[:n_src]
    y_in, dx_in, _, _, y_out, dx_out, a_out, order, wt_buf, xs, dys, ds, os, dxs, y_acc, dx_acc, wt_sem, sems = refs[n_src:]
    i = pl.program_id(0)
    last = pl.num_programs(0) - 1
    row = id_ref[i]
    n_seg = t_ref.shape[0] // SEG
    dim = xs.shape[1]

    def fetch(step):
        lo = 0
        for ref, n in zip(wt_refs, counts):
            @pl.when((step >= lo) & (step < lo + n))
            def _(ref=ref):
                pltpu.make_async_copy(ref.at[src_ref[step]], wt_buf.at[step % 2], wt_sem.at[step % 2]).start()

            lo += n

    def loads():
        return [pltpu.make_async_copy(y_in, y_acc, sems.at[0, 0]), pltpu.make_async_copy(dx_in, dx_acc, sems.at[1, 0])]

    @pl.when(i == 0)
    def _():
        fetch(i)
        if first:
            y_acc[...] = jnp.zeros_like(y_acc)
            dx_acc[...] = jnp.zeros_like(dx_acc)
        else:
            for copy in loads():
                copy.start()
        os[TILE:, :] = jnp.zeros((WIN, dim), BF16)
        dxs[TILE:, :] = jnp.zeros((WIN, dim), BF16)
        order[...] = jnp.zeros_like(order)

    @pl.when(i < last)
    def _():
        fetch(i + 1)

    gather_rows(cnt_ref, row, pos_ref, w_ref, t_ref, xs, dys, ds, n_seg, TILE)
    pltpu.make_async_copy(wt_refs[0].at[0], wt_buf.at[i % 2], wt_sem.at[i % 2]).wait()
    wt = wt_buf.at[pl.ds(i % 2, 1)]
    h, dgu = slot_grads(xs[:TILE, :], ds[:TILE, :], wt, dim)
    os[:TILE, :] = mm(h, wt[0, dim:, :]).astype(BF16)
    dxs[:TILE, :] = mm(dgu, wt[0, :dim, :], 1, 1).astype(BF16)
    if not first:
        @pl.when(i == 0)
        def _():
            for copy in loads():
                copy.wait()

    stores = []
    for b in range(n_seg):
        start0, n_win = window(cnt_ref, row, b)
        tok = slice(b * SEG, (b + 1) * SEG)

        def step(c, a_row, b=b, start0=start0, tok=tok):
            start = pl.multiple_of(start0 + c * WIN, 16)
            hot = hot_rows(pos_ref, b, start)
            sel = hot.astype(F32)
            sel_w = jnp.where(hot, w_ref[0, :, tok], 0.0).astype(BF16)
            o_win = os[pl.ds(start, WIN), :]
            y_acc[tok, :] += mm(sel_w, o_win, 0, 0)
            dx_acc[tok, :] += mm(sel.astype(BF16), dxs[pl.ds(start, WIN), :], 0, 0)
            a_col = jnp.sum(o_win.astype(F32) * dys[pl.ds(start, WIN), :].astype(F32), axis=1, keepdims=True)
            return a_row + jnp.sum(jnp.where(hot, a_col, 0.0), axis=0, keepdims=True)

        a_row = jnp.zeros((1, SEG), F32)
        if EAGER:
            a_row = step(0, a_row)
        a_out[0, :, tok] = lax.fori_loop(int(EAGER), n_win, step, a_row)
        part = pl.ds(b * SEG, SEG)
        done = [pltpu.make_async_copy(y_acc.at[part], y_out.at[part], sems.at[0, b]),
                pltpu.make_async_copy(dx_acc.at[part], dx_out.at[part], sems.at[1, b])]
        stores += done

        @pl.when(i == last)
        def _(done=done):
            for copy in done:
                copy.start()

    @pl.when(i == last)
    def _():
        for copy in stores:
            copy.wait()


def token_side(first, ids, srcs, counts, cnt, pos, w, t, wts, y_in, dx_in, a_in, after):
    n_exp, _, tok_count = pos.shape
    _, w_rows, dim = wts[0].shape
    n_here, n_src = sum(counts), len(counts)
    row_spec = pl.BlockSpec((1, 1, tok_count), lambda i, ids, *_: (ids[i], 0, 0))
    any_spec = pl.BlockSpec(memory_space=pl.ANY)
    acc_shape = jax.ShapeDtypeStruct((tok_count, dim), F32)
    at = 6 + n_src
    return pl.pallas_call(
        functools.partial(token_kernel, first, counts),
        grid_spec=pltpu.PrefetchScalarGridSpec(
            num_scalar_prefetch=3,
            grid=(n_here,),
            in_specs=[row_spec, row_spec, pl.BlockSpec(t.shape, lambda i, *_: (0, 0), pipeline_mode=pl.Buffered(1))]
            + [any_spec] * (n_src + 4),
            out_specs=[any_spec, any_spec, row_spec, pl.BlockSpec((8, 128), lambda i, *_: (0, 0))],
            scratch_shapes=[pltpu.VMEM((2, w_rows, dim), BF16)] + [pltpu.VMEM((TILE + WIN, dim), BF16)] * 5
            + [pltpu.VMEM((tok_count, dim), F32)] * 2
            + [pltpu.SemaphoreType.DMA((2,)), pltpu.SemaphoreType.DMA((2, tok_count // SEG))],
        ),
        out_shape=[acc_shape, acc_shape, jax.ShapeDtypeStruct((n_exp, 1, tok_count), F32), jax.ShapeDtypeStruct((8, 128), F32)],
        input_output_aliases={at + 2: 2} if first else {at: 0, at + 1: 1, at + 2: 2},
        compiler_params=pltpu.CompilerParams(dimension_semantics=("arbitrary",), vmem_limit_bytes=67000000),
        cost_estimate=pl.CostEstimate(flops=n_here * 2 * 4 * 640 * w_rows * dim, bytes_accessed=50 << 20, transcendentals=0),
        name="token_side",
    )(ids, srcs, cnt, pos, w, t, *wts, y_in, dx_in, a_in, after)


def owner_kernel(first, cnt_ref, pos_ref, w_ref, t_ref, wt_ref, acc_in, after, acc_out, order, xs, ds, acc, sem):
    g, e = pl.program_id(0), pl.program_id(1)
    n_grp, n_exp = pl.num_programs(0), pl.num_programs(1)
    n_seg = t_ref.shape[0] // SEG
    dim = xs.shape[1]
    row = g * n_exp + e

    @pl.when((g == 0) & (e == 0))
    def _():
        if first:
            acc[...] = jnp.zeros_like(acc)
        else:
            for k in range(acc.shape[0]):
                pltpu.make_async_copy(acc_in.at[k], acc.at[k], sem.at[k]).start()
        order[...] = jnp.zeros_like(order)

    n_tile = (cnt_ref[row, n_seg] + TILE - 1) // TILE
    gather_rows(cnt_ref, row, pos_ref, w_ref, t_ref, xs, None, ds, n_seg, n_tile * TILE)
    if not first:
        @pl.when(g == 0)
        def _():
            pltpu.make_async_copy(acc_in.at[e], acc.at[e], sem.at[e]).wait()

    def tile(t, _):
        at = pl.multiple_of(t * TILE, 16)
        x, d = xs[pl.ds(at, TILE), :], ds[pl.ds(at, TILE), :]
        h, dgu = slot_grads(x, d, wt_ref, dim)
        acc[e, dim:, :] += mm(h, d, 0, 0)
        acc[e, :dim, :] += mm(x, dgu, 0, 0)
        return 0

    lax.fori_loop(0, n_tile, tile, 0)

    @pl.when(g == n_grp - 1)
    def _():
        pltpu.make_async_copy(acc.at[e], acc_out.at[e], sem.at[e]).start()

    @pl.when((g == n_grp - 1) & (e == n_exp - 1))
    def _():
        for k in range(acc.shape[0]):
            pltpu.make_async_copy(acc.at[k], acc_out.at[k], sem.at[k]).wait()


def owner_side(first, cnt, pos, w, t, wt, acc, after):
    n_exp, w_rows, dim = wt.shape
    grp = pos.shape[2]
    n_grp = t.shape[0] // grp
    per_row = pl.BlockSpec((1, 1, grp), lambda g, e, c: (g * n_exp + e, 0, 0))
    any_spec = pl.BlockSpec(memory_space=pl.ANY)
    rows = -(-grp // TILE) * TILE + WIN
    return pl.pallas_call(
        functools.partial(owner_kernel, first),
        grid_spec=pltpu.PrefetchScalarGridSpec(
            num_scalar_prefetch=1,
            grid=(n_grp, n_exp),
            in_specs=[per_row, per_row, pl.BlockSpec((grp, t.shape[1]), lambda g, e, c: (g, 0)),
                      pl.BlockSpec((1, w_rows, dim), lambda g, e, c: (e, 0, 0)), any_spec, any_spec],
            out_specs=[any_spec, pl.BlockSpec((8, 128), lambda g, e, c: (0, 0))],
            scratch_shapes=[pltpu.VMEM((rows, dim), BF16)] * 2
            + [pltpu.VMEM((n_exp, w_rows, dim), F32), pltpu.SemaphoreType.DMA((n_exp,))],
        ),
        out_shape=[jax.ShapeDtypeStruct(wt.shape, F32), jax.ShapeDtypeStruct((8, 128), F32)],
        input_output_aliases={} if first else {5: 0},
        compiler_params=pltpu.CompilerParams(dimension_semantics=("arbitrary", "arbitrary"), vmem_limit_bytes=67000000),
        cost_estimate=pl.CostEstimate(flops=n_grp * n_exp * 2 * 4 * 640 * w_rows * dim, bytes_accessed=50 << 20, transcendentals=0),
        name="owner_side",
    )(cnt, pos, w, t, wt, acc, after)


def running_count(hot):
    rows, width = hot.shape
    blocks = hot.reshape(rows, width // 256, 256)
    upper = (jnp.arange(256)[:, None] < jnp.arange(256)[None, :]).astype(BF16)
    inside = jnp.einsum("rbi,ij->rbj", blocks.astype(BF16), upper, preferred_element_type=F32)
    total = jnp.sum(blocks, axis=2)
    n_blk = width // 256
    before = jnp.sum(jnp.where(jnp.arange(n_blk)[:, None] < jnp.arange(n_blk + 1)[None, :], total[:, :, None], 0.0), axis=1)
    return (inside + before[:, :-1, None]).reshape(rows, width), before[:, ::SEG // 256]


def solution(mesh):
    n_dev = mesh.shape["ep"]
    planes = [[d for d in range(n_dev) if d // 2 % 2 == x] for x in range(2)]
    across = [(d, d ^ 2) for d in range(n_dev)]
    beside = [(d, d ^ 1) for d in range(n_dev)]
    n_plane = n_dev // 2

    def local_block(x_loc, w_router, wg_loc, wu_loc, wd_loc, idx_loc, dy_loc):
        tok_count, dim = x_loc.shape
        top_k = idx_loc.shape[1]
        n_exp = w_router.shape[1]
        loc_exp = wg_loc.shape[0]
        ff = wg_loc.shape[2]
        capacity = (5 * tok_count * top_k + 4 * n_exp - 1) // (4 * n_exp)
        n_total = tok_count * n_dev
        n_half = 2
        span = tok_count // n_half
        me = lax.axis_index("ep")
        my_chip, my_x, my_core = me // 4, me // 2 % 2, me % 2
        share = lambda a: lax.all_to_all(jnp.broadcast_to(a, (n_dev,) + a.shape), "ep", 0, 0)
        plane_gather = lambda a: lax.all_gather(a, "ep", axis=0, tiled=True, axis_index_groups=planes)

        t_loc = jnp.concatenate([x_loc, dy_loc], axis=1)
        wt_loc = jnp.concatenate([jnp.concatenate([wg_loc, wu_loc], axis=2), wd_loc], axis=1)
        wt_nbr = lax.ppermute(wt_loc, "ep", across)
        wt_par = lax.ppermute(wt_loc, "ep", beside)
        nbr_par = lax.ppermute(wt_nbr[:1], "ep", beside)
        odd_plane = plane_gather(wt_loc[1:])
        t_all = [plane_gather(t_loc[c * span:(c + 1) * span]) for c in range(n_half)]
        even_plane = plane_gather(wt_loc[:1])
        even_nbr = plane_gather(wt_nbr[:1])
        mine = lax.dynamic_slice_in_dim(odd_plane, my_core * (n_plane // 2), n_plane // 2, 0)
        odd_nbr = lax.ppermute(mine, "ep", across)
        odd_nbr_par = lax.ppermute(odd_nbr, "ep", beside)

        idx_t = idx_loc.T
        exp_id = jnp.arange(n_exp, dtype=jnp.int32)[:, None]
        hot = exp_id == idx_t[0:1]
        for k in range(1, top_k):
            hot = hot | (exp_id == idx_t[k:k + 1])
        logits = lax.dot_general(w_router, x_loc, (((0,), (1,)), ((), ())), preferred_element_type=F32)
        prob = jax.nn.softmax(logits, axis=0)
        pick_sum = jnp.sum(jnp.where(hot, prob, 0.0), axis=0, keepdims=True)
        gate = jnp.where(hot, prob / pick_sum, 0.0)
        gate_bf = lax.reduce_precision(gate, 8, 7)
        earlier, before = running_count(hot.astype(F32))
        kept = hot & (earlier < capacity)
        pos = jnp.where(kept, earlier, -1.0).astype(jnp.int32)[:, None, :]
        cnt = jnp.minimum(before, capacity).astype(jnp.int32)

        sent = jnp.where(kept, gate_bf, -1.0).reshape(n_plane // 2, 2, 2, loc_exp, tok_count)
        sent = sent.transpose(0, 2, 1, 3, 4).reshape(n_plane, 2 * loc_exp, tok_count)
        got = lax.all_to_all(sent, "ep", 0, 0, axis_index_groups=planes)
        got = got.reshape(n_plane // n_half, n_half, 2, loc_exp, n_half, span).transpose(2, 4, 0, 3, 1, 5)
        got = jnp.where(my_x == 0, got[::-1], got).reshape(-1, tok_count)
        own_hot = got >= 0.0
        own_pos, own_cnt = running_count(own_hot.astype(F32))
        own_pos = jnp.where(own_hot, own_pos, -1.0).astype(jnp.int32)[:, None, :]
        own_cnt = own_cnt.astype(jnp.int32)
        own_w = jnp.where(own_hot, got, 0.0)[:, None, :]
        n_row = own_pos.shape[0] // (2 * n_half)

        zero = jnp.zeros((8, 128), F32)
        state = [zero, zero, jnp.zeros((n_exp, 1, tok_count), F32), zero]
        rest = jnp.arange(2 * n_plane // 2 - 2, dtype=jnp.int32)
        rest = (my_chip ^ (rest // 2 + 1)) * 2 + rest % 2
        expert = lambda place, x, j: (place // 2 * 4 + 2 * x + place % 2) * loc_exp + j
        quarter = jnp.arange(n_plane // 2, dtype=jnp.int32)
        pair = jnp.arange(loc_exp, dtype=jnp.int32)
        row_w = gate_bf[:, None, :]

        def run_token(parts, state):
            ids = jnp.concatenate([p[1] for p in parts])
            srcs = jnp.concatenate([p[2] for p in parts])
            counts = tuple(p[1].shape[0] for p in parts)
            first = state[0].shape == zero.shape
            return token_side(first, ids, srcs, counts, cnt, pos, row_w, t_loc, [p[0] for p in parts], *state)

        one = jnp.zeros((1,), jnp.int32)
        state = run_token([(wt_loc, me * loc_exp + pair, pair), (wt_par, (me ^ 1) * loc_exp + pair, pair)], state)
        state = run_token([(odd_plane, expert(rest, my_x, 1), rest), (wt_nbr, (me ^ 2) * loc_exp + one, one),
                           (nbr_par, (me ^ 3) * loc_exp + one, one)], state)
        sums = [zero, zero]
        order = state[3]
        for c in range(n_half):
            for p, wt in enumerate((wt_nbr, wt_loc)):
                part = slice((p * n_half + c) * n_row, (p * n_half + c + 1) * n_row)
                sums[p], order = owner_side(c == 0, own_cnt[part], own_pos[part], own_w[part], t_all[c], wt, sums[p], order)
        from_nbr = lax.ppermute(sums[0], "ep", across)
        half = n_plane // 2
        state = run_token([(odd_nbr, expert(my_core * half + quarter, 1 - my_x, 1), quarter),
                           (odd_nbr_par, expert((1 - my_core) * half + quarter, 1 - my_x, 1), quarter),
                           (even_plane, expert(rest, my_x, 0), rest)], [*state[:3], order])
        y_acc, dx_acc, a, _ = run_token([(even_nbr, expert(rest, 1 - my_x, 0), rest)], state)
        a = a[:, 0]

        load_stats = jnp.concatenate([jnp.sum(hot.astype(F32), axis=1), jnp.sum(prob, axis=1)])
        load_stats = jnp.sum(share(load_stats), axis=0)
        load_frac = load_stats[:n_exp] / (n_total * top_k)
        mean_prob = load_stats[n_exp:] / n_total
        aux_loss = AUX_COEF * n_exp * jnp.sum(load_frac * mean_prob)

        d_pick = (a - jnp.sum(a * gate, axis=0, keepdims=True)) / pick_sum
        d_prob = jnp.where(hot, d_pick, 0.0) + (AUX_COEF * n_exp / n_total) * load_frac[:, None]
        d_logit = (prob * (d_prob - jnp.sum(prob * d_prob, axis=0, keepdims=True))).astype(BF16)
        dw_router = lax.dot_general(d_logit, x_loc, (((1,), (0,)), ((), ())), preferred_element_type=F32)
        parts = lax.all_to_all(dw_router.reshape(n_exp, n_dev, dim // n_dev).transpose(1, 0, 2), "ep", 0, 0)
        dw_router = share(jnp.sum(parts, axis=0).T).reshape(dim, n_exp)
        dx_router = lax.dot_general(d_logit, w_router, (((0,), (1,)), ((), ())), preferred_element_type=F32)
        dw = sums[1] + from_nbr
        return (y_acc.astype(BF16), aux_loss, (dx_acc + dx_router).astype(BF16), dw_router,
                dw[:, :dim, :ff], dw[:, :dim, ff:], dw[:, dim:])

    tok_spec = P("ep")
    return jax.shard_map(
        local_block,
        mesh=mesh,
        in_specs=(tok_spec, P(), tok_spec, tok_spec, tok_spec, tok_spec, tok_spec),
        out_specs=(tok_spec, P(), tok_spec, P(), tok_spec, tok_spec, tok_spec),
        check_vma=False,
    )
```

```python
import functools

import jax
import jax.numpy as jnp
from jax import lax
from jax.experimental import pallas as pl
from jax.experimental.pallas import tpu as pltpu
from jax.sharding import PartitionSpec as P


AUX_COEF = 0.001
SEG = 512
WIN = 176
SMALL, TILE = 512, 640
F32, BF16 = jnp.float32, jnp.bfloat16


def mm(a, b, ca=1, cb=0):
    return lax.dot_general(a, b, (((ca,), (cb,)), ((), ())), preferred_element_type=F32)


def window(cnt_ref, row, b):
    start = (cnt_ref[row, b] // 16) * 16
    return pl.multiple_of(start, 16), jnp.maximum((cnt_ref[row, b + 1] - start + WIN - 1) // WIN, 1)


def hot_rows(pos_row, b, start):
    pos = pos_row[:, b * SEG:(b + 1) * SEG] - start
    return lax.broadcasted_iota(jnp.int32, (WIN, SEG), 0) == pos


def gather_rows(cnt_ref, experts, t_ref, n_seg):
    dim = experts[0][3].shape[1]
    ends = [0] * len(experts)
    for b in range(n_seg):
        spans = [window(cnt_ref, ex[0], b) for ex in experts]
        tok = slice(b * SEG, (b + 1) * SEG)

        def step(c, _, b=b, spans=spans, tok=tok, eager=False):
            starts = [pl.multiple_of(first + c * WIN, 16) for first, _ in spans]
            hots = [hot_rows(ex[1], b, start) for ex, start in zip(experts, starts)]
            sel = jnp.concatenate([hot.astype(F32).astype(BF16) for hot in hots], axis=0)
            both = mm(sel, t_ref[tok, :])
            for k, ((row, _, w_row, xs, dys, ds, _), start, hot) in enumerate(zip(experts, starts, hots)):
                rows = slice(k * WIN, (k + 1) * WIN)

                def store(row=row, w_row=w_row, xs=xs, dys=dys, ds=ds, start=start, hot=hot, rows=rows):
                    x_new, dy_new = both[rows, :dim], both[rows, dim:]
                    w_col = jnp.sum(jnp.where(hot, w_row[:, tok], 0.0), axis=1, keepdims=True)
                    outs = [(xs, x_new), (ds, w_col * dy_new)] + ([(dys, dy_new)] if dys is not None else [])
                    for ref, new in outs:
                        new = new.astype(BF16)
                        ref[pl.ds(start + 16, WIN - 16), :] = new[16:]
                        if b == 0 or not eager:
                            ref[pl.ds(start, 16), :] = new[:16]
                        else:
                            head = lax.broadcasted_iota(jnp.int32, (16, dim), 0) < cnt_ref[row, b] - start
                            old = ref[pl.ds(start, 16), :].astype(F32)
                            ref[pl.ds(start, 16), :] = jnp.where(head, old, new[:16].astype(F32)).astype(BF16)

                if eager:
                    store()
                else:
                    pl.when(c < spans[k][1])(store)
            return 0

        step(0, 0, eager=True)
        lax.fori_loop(1, functools.reduce(jnp.maximum, [n for _, n in spans]), step, 0)
        ends = [first + n * WIN for first, n in spans]

    for (_, _, _, xs, dys, ds, n_rows), end in zip(experts, ends):
        def clear(i, _, xs=xs, dys=dys, ds=ds):
            at = pl.ds(pl.multiple_of(i * 16, 16), 16)
            zero = jnp.zeros((16, dim), BF16)
            for ref in (xs, dys, ds):
                if ref is not None:
                    ref[at, :] = zero
            return 0

        lax.fori_loop(end // 16, n_rows // 16, clear, 0)


def slot_grads(x, d, w_ref, dim):
    pre = mm(x, w_ref[0, :dim, :])
    ff = pre.shape[1] // 2
    g, u = pre[:, :ff], pre[:, ff:]
    s = jax.nn.sigmoid(g)
    act = g * s
    h = (act * u).astype(BF16)
    dh = mm(d, w_ref[0, dim:, :], 1, 1).astype(BF16).astype(F32)
    dg = (dh * u * s * (1.0 + g * (1.0 - s))).astype(BF16)
    du = (dh * act).astype(BF16)
    return h, jnp.concatenate([dg, du], axis=1)


def token_kernel(first, counts, id_ref, src_ref, cnt_ref, pos_ref, w_ref, pos2_ref, w2_ref, t_ref, *refs):
    n_src = len(counts)
    wt_refs = refs[:n_src]
    y_in, dx_in, _, _, y_out, dx_out, a_out, order, wt_buf, xs, dys, ds, os, dxs, y_acc, dx_acc, wt_sem, sems = refs[n_src:]
    i = pl.program_id(0)
    last = pl.num_programs(0) - 1
    row = id_ref[i]
    n_seg = t_ref.shape[0] // SEG
    dim = xs.shape[2]

    def fetch(step):
        lo = 0
        for ref, n in zip(wt_refs, counts):
            @pl.when((step >= lo) & (step < lo + n))
            def _(ref=ref):
                pltpu.make_async_copy(ref.at[src_ref[step]], wt_buf.at[step % 2], wt_sem.at[step % 2]).start()

            lo += n

    def loads():
        return [pltpu.make_async_copy(y_in, y_acc, sems.at[0, 0]), pltpu.make_async_copy(dx_in, dx_acc, sems.at[1, 0])]

    @pl.when(i == 0)
    def _():
        fetch(i)
        if first:
            y_acc[...] = jnp.zeros_like(y_acc)
            dx_acc[...] = jnp.zeros_like(dx_acc)
        else:
            for copy in loads():
                copy.start()
        os[TILE:, :] = jnp.zeros((WIN, dim), BF16)
        dxs[TILE:, :] = jnp.zeros((WIN, dim), BF16)
        order[...] = jnp.zeros_like(order)

    @pl.when(i < last)
    def _():
        fetch(i + 1)

    @pl.when(i % 2 == 0)
    def _():
        gather_rows(cnt_ref, [(row, pos_ref[0], w_ref[0], xs.at[0], dys.at[0], ds.at[0], TILE),
                              (id_ref[i + 1], pos2_ref[0], w2_ref[0], xs.at[1], dys.at[1], ds.at[1], TILE)], t_ref, n_seg)

    xs, dys, ds = xs.at[i % 2], dys.at[i % 2], ds.at[i % 2]
    pltpu.make_async_copy(wt_refs[0].at[0], wt_buf.at[i % 2], wt_sem.at[i % 2]).wait()
    wt = wt_buf.at[pl.ds(i % 2, 1)]

    def experts_mlp(rows):
        h, dgu = slot_grads(xs[:rows, :], ds[:rows, :], wt, dim)
        os[:rows, :] = mm(h, wt[0, dim:, :]).astype(BF16)
        dxs[:rows, :] = mm(dgu, wt[0, :dim, :], 1, 1).astype(BF16)

    @pl.when(cnt_ref[row, n_seg] <= SMALL)
    def _():
        experts_mlp(SMALL)
        os[SMALL:SMALL + WIN, :] = jnp.zeros((WIN, dim), BF16)
        dxs[SMALL:SMALL + WIN, :] = jnp.zeros((WIN, dim), BF16)

    @pl.when(cnt_ref[row, n_seg] > SMALL)
    def _():
        experts_mlp(TILE)

    if not first:
        @pl.when(i == 0)
        def _():
            for copy in loads():
                copy.wait()

    stores = []
    for b in range(n_seg):
        start0, n_win = window(cnt_ref, row, b)
        tok = slice(b * SEG, (b + 1) * SEG)

        def step(c, a_row, b=b, start0=start0, tok=tok):
            start = pl.multiple_of(start0 + c * WIN, 16)
            hot = hot_rows(pos_ref[0], b, start)
            sel = hot.astype(F32)
            sel_w = jnp.where(hot, w_ref[0, :, tok], 0.0).astype(BF16)
            o_win = os[pl.ds(start, WIN), :]
            y_acc[tok, :] += mm(sel_w, o_win, 0, 0)
            dx_acc[tok, :] += mm(sel.astype(BF16), dxs[pl.ds(start, WIN), :], 0, 0)
            a_col = jnp.sum(o_win.astype(F32) * dys[pl.ds(start, WIN), :].astype(F32), axis=1, keepdims=True)
            return a_row + jnp.sum(jnp.where(hot, a_col, 0.0), axis=0, keepdims=True)

        a_row = step(0, jnp.zeros((1, SEG), F32))
        a_out[0, :, tok] = lax.fori_loop(1, n_win, step, a_row)
        part = pl.ds(b * SEG, SEG)
        done = [pltpu.make_async_copy(y_acc.at[part], y_out.at[part], sems.at[0, b]),
                pltpu.make_async_copy(dx_acc.at[part], dx_out.at[part], sems.at[1, b])]
        stores += done

        @pl.when(i == last)
        def _(done=done):
            for copy in done:
                copy.start()

    @pl.when(i == last)
    def _():
        for copy in stores:
            copy.wait()


def token_side(first, ids, srcs, counts, cnt, pos, w, t, wts, y_in, dx_in, a_in, after):
    n_exp, _, tok_count = pos.shape
    _, w_rows, dim = wts[0].shape
    n_here, n_src = sum(counts), len(counts)
    row_spec = pl.BlockSpec((1, 1, tok_count), lambda i, ids, *_: (ids[i], 0, 0))
    next_spec = pl.BlockSpec((1, 1, tok_count), lambda i, ids, *_: (ids[i // 2 * 2 + 1], 0, 0))
    any_spec = pl.BlockSpec(memory_space=pl.ANY)
    acc_shape = jax.ShapeDtypeStruct((tok_count, dim), F32)
    at = 8 + n_src
    return pl.pallas_call(
        functools.partial(token_kernel, first, counts),
        grid_spec=pltpu.PrefetchScalarGridSpec(
            num_scalar_prefetch=3,
            grid=(n_here,),
            in_specs=[row_spec, row_spec, next_spec, next_spec, pl.BlockSpec(t.shape, lambda i, *_: (0, 0), pipeline_mode=pl.Buffered(1))]
            + [any_spec] * (n_src + 4),
            out_specs=[any_spec, any_spec, row_spec, pl.BlockSpec((8, 128), lambda i, *_: (0, 0))],
            scratch_shapes=[pltpu.VMEM((2, w_rows, dim), BF16)] + [pltpu.VMEM((2, TILE + WIN, dim), BF16)] * 3
            + [pltpu.VMEM((TILE + WIN, dim), BF16)] * 2
            + [pltpu.VMEM((tok_count, dim), F32)] * 2
            + [pltpu.SemaphoreType.DMA((2,)), pltpu.SemaphoreType.DMA((2, tok_count // SEG))],
        ),
        out_shape=[acc_shape, acc_shape, jax.ShapeDtypeStruct((n_exp, 1, tok_count), F32), jax.ShapeDtypeStruct((8, 128), F32)],
        input_output_aliases={at + 2: 2} if first else {at: 0, at + 1: 1, at + 2: 2},
        compiler_params=pltpu.CompilerParams(dimension_semantics=("arbitrary",), vmem_limit_bytes=67000000),
        cost_estimate=pl.CostEstimate(flops=n_here * 2 * 4 * 640 * w_rows * dim, bytes_accessed=50 << 20, transcendentals=0),
        name="token_side",
    )(ids, srcs, cnt, pos, w, pos, w, t, *wts, y_in, dx_in, a_in, after)


def owner_kernel(first, cnt_ref, pos_ref, w_ref, t_ref, wt_ref, acc_in, after, acc_out, order, xs, ds, acc, sem):
    g, e = pl.program_id(0), pl.program_id(1)
    n_grp, n_exp = pl.num_programs(0), pl.num_programs(1)
    n_seg = t_ref.shape[0] // SEG
    dim = xs.shape[2]
    row = g * n_exp + e

    @pl.when((g == 0) & (e == 0))
    def _():
        if first:
            acc[...] = jnp.zeros_like(acc)
        else:
            for k in range(acc.shape[0]):
                pltpu.make_async_copy(acc_in.at[k], acc.at[k], sem.at[k]).start()
        order[...] = jnp.zeros_like(order)

    def n_tile(k):
        return jnp.maximum((cnt_ref[g * n_exp + k, n_seg] + TILE - 1) // TILE, 1)

    @pl.when(e == 0)
    def _():
        gather_rows(cnt_ref, [(g * n_exp + k, pos_ref[k], w_ref[k], xs.at[k], None, ds.at[k], n_tile(k) * TILE)
                              for k in range(xs.shape[0])], t_ref, n_seg)

    if not first:
        @pl.when(g == 0)
        def _():
            pltpu.make_async_copy(acc_in.at[e], acc.at[e], sem.at[e]).wait()

    def tile(t, rows=TILE):
        at = pl.ds(pl.multiple_of(t * rows, 16), rows)
        x, d = xs[e, at, :], ds[e, at, :]
        h, dgu = slot_grads(x, d, wt_ref, dim)
        acc[e, dim:, :] += mm(h, d, 0, 0)
        acc[e, :dim, :] += mm(x, dgu, 0, 0)

    def large(t, _):
        tile(t)
        return 0

    count = cnt_ref[row, n_seg]
    pl.when(count <= SMALL)(lambda: tile(0, SMALL))
    lax.fori_loop(0, jnp.where(count <= SMALL, 0, n_tile(e)), large, 0)

    @pl.when(g == n_grp - 1)
    def _():
        pltpu.make_async_copy(acc.at[e], acc_out.at[e], sem.at[e]).start()

    @pl.when((g == n_grp - 1) & (e == n_exp - 1))
    def _():
        for k in range(acc.shape[0]):
            pltpu.make_async_copy(acc.at[k], acc_out.at[k], sem.at[k]).wait()


def owner_side(first, max_rows, cnt, pos, w, t, wt, acc, after):
    n_exp, w_rows, dim = wt.shape
    grp = pos.shape[2]
    n_grp = t.shape[0] // grp
    per_row = pl.BlockSpec((n_exp, 1, grp), lambda g, e, c: (g, 0, 0))
    any_spec = pl.BlockSpec(memory_space=pl.ANY)
    rows = -(-max_rows // TILE) * TILE + WIN
    return pl.pallas_call(
        functools.partial(owner_kernel, first),
        grid_spec=pltpu.PrefetchScalarGridSpec(
            num_scalar_prefetch=1,
            grid=(n_grp, n_exp),
            in_specs=[per_row, per_row, pl.BlockSpec((grp, t.shape[1]), lambda g, e, c: (g, 0)),
                      pl.BlockSpec((1, w_rows, dim), lambda g, e, c: (e, 0, 0)), any_spec, any_spec],
            out_specs=[any_spec, pl.BlockSpec((8, 128), lambda g, e, c: (0, 0))],
            scratch_shapes=[pltpu.VMEM((n_exp, rows, dim), BF16)] * 2
            + [pltpu.VMEM((n_exp, w_rows, dim), F32), pltpu.SemaphoreType.DMA((n_exp,))],
        ),
        out_shape=[jax.ShapeDtypeStruct(wt.shape, F32), jax.ShapeDtypeStruct((8, 128), F32)],
        input_output_aliases={} if first else {5: 0},
        compiler_params=pltpu.CompilerParams(dimension_semantics=("arbitrary", "arbitrary"), vmem_limit_bytes=67000000),
        cost_estimate=pl.CostEstimate(flops=n_grp * n_exp * 2 * 4 * 640 * w_rows * dim, bytes_accessed=50 << 20, transcendentals=0),
        name="owner_side",
    )(cnt, pos, w, t, wt, acc, after)


def running_count(hot):
    rows, width = hot.shape
    blocks = hot.reshape(rows, width // 256, 256)
    upper = (jnp.arange(256)[:, None] < jnp.arange(256)[None, :]).astype(BF16)
    inside = jnp.einsum("rbi,ij->rbj", blocks.astype(BF16), upper, preferred_element_type=F32)
    total = jnp.sum(blocks, axis=2)
    n_blk = width // 256
    before = jnp.sum(jnp.where(jnp.arange(n_blk)[:, None] < jnp.arange(n_blk + 1)[None, :], total[:, :, None], 0.0), axis=1)
    return (inside + before[:, :-1, None]).reshape(rows, width), before[:, ::SEG // 256]


def solution(mesh):
    n_dev = mesh.shape["ep"]
    planes = [[d for d in range(n_dev) if d // 2 % 2 == x] for x in range(2)]
    across = [(d, d ^ 2) for d in range(n_dev)]
    beside = [(d, d ^ 1) for d in range(n_dev)]
    n_plane = n_dev // 2

    def local_block(x_loc, w_router, wg_loc, wu_loc, wd_loc, idx_loc, dy_loc):
        tok_count, dim = x_loc.shape
        top_k = idx_loc.shape[1]
        n_exp = w_router.shape[1]
        loc_exp = wg_loc.shape[0]
        ff = wg_loc.shape[2]
        capacity = (5 * tok_count * top_k + 4 * n_exp - 1) // (4 * n_exp)
        n_total = tok_count * n_dev
        n_half = 2
        span = tok_count // n_half
        me = lax.axis_index("ep")
        my_chip, my_x, my_core = me // 4, me // 2 % 2, me % 2
        share = lambda a: lax.all_to_all(jnp.broadcast_to(a, (n_dev,) + a.shape), "ep", 0, 0)
        plane_gather = lambda a: lax.all_gather(a, "ep", axis=0, tiled=True, axis_index_groups=planes)

        t_loc = jnp.concatenate([x_loc, dy_loc], axis=1)
        wt_loc = jnp.concatenate([jnp.concatenate([wg_loc, wu_loc], axis=2), wd_loc], axis=1)
        wt_nbr = lax.ppermute(wt_loc, "ep", across)
        wt_par = lax.ppermute(wt_loc, "ep", beside)
        nbr_par = lax.ppermute(wt_nbr[:1], "ep", beside)
        odd_plane = plane_gather(wt_loc[1:])
        t_all = [plane_gather(t_loc[c * span:(c + 1) * span]) for c in range(n_half)]
        even_plane = plane_gather(wt_loc[:1])
        even_nbr = plane_gather(wt_nbr[:1])
        mine = lax.dynamic_slice_in_dim(odd_plane, my_core * (n_plane // 2), n_plane // 2, 0)
        odd_nbr = lax.ppermute(mine, "ep", across)
        odd_nbr_par = lax.ppermute(odd_nbr, "ep", beside)

        idx_t = idx_loc.T
        exp_id = jnp.arange(n_exp, dtype=jnp.int32)[:, None]
        hot = exp_id == idx_t[0:1]
        for k in range(1, top_k):
            hot = hot | (exp_id == idx_t[k:k + 1])
        logits = lax.dot_general(w_router, x_loc, (((0,), (1,)), ((), ())), preferred_element_type=F32)
        prob = jax.nn.softmax(logits, axis=0)
        pick_sum = jnp.sum(jnp.where(hot, prob, 0.0), axis=0, keepdims=True)
        gate = jnp.where(hot, prob / pick_sum, 0.0)
        gate_bf = lax.reduce_precision(gate, 8, 7)
        earlier, before = running_count(hot.astype(F32))
        kept = hot & (earlier < capacity)
        pos = jnp.where(kept, earlier, -1.0).astype(jnp.int32)[:, None, :]
        cnt = jnp.minimum(before, capacity).astype(jnp.int32)

        sent = jnp.where(kept, gate_bf, -1.0).reshape(n_plane // 2, 2, 2, loc_exp, tok_count)
        sent = sent.transpose(0, 2, 1, 3, 4).reshape(n_plane, 2 * loc_exp, tok_count)
        got = lax.all_to_all(sent, "ep", 0, 0, axis_index_groups=planes)
        got = got.reshape(n_plane // n_half, n_half, 2, loc_exp, n_half, span).transpose(2, 4, 0, 3, 1, 5)
        got = jnp.where(my_x == 0, got[::-1], got).reshape(-1, tok_count)
        own_hot = got >= 0.0
        own_pos, own_cnt = running_count(own_hot.astype(F32))
        own_pos = jnp.where(own_hot, own_pos, -1.0).astype(jnp.int32)[:, None, :]
        own_cnt = own_cnt.astype(jnp.int32)
        own_w = jnp.where(own_hot, got, 0.0)[:, None, :]
        n_row = own_pos.shape[0] // (2 * n_half)

        zero = jnp.zeros((8, 128), F32)
        state = [zero, zero, jnp.zeros((n_exp, 1, tok_count), F32), zero]
        rest = jnp.arange(2 * n_plane // 2 - 2, dtype=jnp.int32)
        rest = (my_chip ^ (rest // 2 + 1)) * 2 + rest % 2
        expert = lambda place, x, j: (place // 2 * 4 + 2 * x + place % 2) * loc_exp + j
        quarter = jnp.arange(n_plane // 2, dtype=jnp.int32)
        pair = jnp.arange(loc_exp, dtype=jnp.int32)
        row_w = gate_bf[:, None, :]

        def run_token(parts, state):
            ids = jnp.concatenate([p[1] for p in parts])
            srcs = jnp.concatenate([p[2] for p in parts])
            counts = tuple(p[1].shape[0] for p in parts)
            first = state[0].shape == zero.shape
            return token_side(first, ids, srcs, counts, cnt, pos, row_w, t_loc, [p[0] for p in parts], *state)

        one = jnp.zeros((1,), jnp.int32)
        state = run_token([(wt_loc, me * loc_exp + pair, pair), (wt_par, (me ^ 1) * loc_exp + pair, pair)], state)
        state = run_token([(odd_plane, expert(rest, my_x, 1), rest), (wt_nbr, (me ^ 2) * loc_exp + one, one),
                           (nbr_par, (me ^ 3) * loc_exp + one, one)], state)
        sums = [zero, zero]
        order = state[3]
        for c in range(n_half):
            for p, wt in enumerate((wt_nbr, wt_loc)):
                part = slice((p * n_half + c) * n_row, (p * n_half + c + 1) * n_row)
                sums[p], order = owner_side(c == 0, min(n_half * capacity, tok_count), own_cnt[part], own_pos[part], own_w[part], t_all[c], wt, sums[p], order)
        from_nbr = lax.ppermute(sums[0], "ep", across)
        half = n_plane // 2
        state = run_token([(odd_nbr, expert(my_core * half + quarter, 1 - my_x, 1), quarter),
                           (odd_nbr_par, expert((1 - my_core) * half + quarter, 1 - my_x, 1), quarter),
                           (even_plane, expert(rest, my_x, 0), rest)], [*state[:3], order])
        y_acc, dx_acc, a, _ = run_token([(even_nbr, expert(rest, 1 - my_x, 0), rest)], state)
        a = a[:, 0]

        load_stats = jnp.concatenate([jnp.sum(hot.astype(F32), axis=1), jnp.sum(prob, axis=1)])
        load_stats = jnp.sum(share(load_stats), axis=0)
        load_frac = load_stats[:n_exp] / (n_total * top_k)
        mean_prob = load_stats[n_exp:] / n_total
        aux_loss = AUX_COEF * n_exp * jnp.sum(load_frac * mean_prob)

        d_pick = (a - jnp.sum(a * gate, axis=0, keepdims=True)) / pick_sum
        d_prob = jnp.where(hot, d_pick, 0.0) + (AUX_COEF * n_exp / n_total) * load_frac[:, None]
        d_logit = (prob * (d_prob - jnp.sum(prob * d_prob, axis=0, keepdims=True))).astype(BF16)
        dw_router = lax.dot_general(d_logit, x_loc, (((1,), (0,)), ((), ())), preferred_element_type=F32)
        parts = lax.all_to_all(dw_router.reshape(n_exp, n_dev, dim // n_dev).transpose(1, 0, 2), "ep", 0, 0)
        dw_router = share(jnp.sum(parts, axis=0).T).reshape(dim, n_exp)
        dx_router = lax.dot_general(d_logit, w_router, (((0,), (1,)), ((), ())), preferred_element_type=F32)
        joined = lambda rows, cols: sums[1][:, rows, cols] + from_nbr[:, rows, cols]
        top, low = slice(0, dim), slice(dim, None)
        return (y_acc.astype(BF16), aux_loss, (dx_acc + dx_router).astype(BF16), dw_router,
                joined(top, slice(0, ff)), joined(top, slice(ff, None)), joined(low, slice(None)))

    tok_spec = P("ep")
    return jax.shard_map(
        local_block,
        mesh=mesh,
        in_specs=(tok_spec, P(), tok_spec, tok_spec, tok_spec, tok_spec, tok_spec),
        out_specs=(tok_spec, P(), tok_spec, P(), tok_spec, tok_spec, tok_spec),
        check_vma=False,
    )
```
